256 devices in a mesh: expert: 128 (over x_hi, y, z, core), tensor: 2 (over x_lo).
Axes of the slice: x: 4 (x_hi: 2, x_lo: 2; x = x_hi * 2 + x_lo), y: 4, z: 8, core: 2. Of those that a mesh axis runs over, the one named last changes fastest.
Arguments:
- tokens: bfloat16 [65536, 768], P(('expert', 'tensor')), may hold values from -6 to 6
- norm_gain: float32 [768], replicated, may hold values from 0.25 to 1.75
- gates: float32 [65536], P(('expert', 'tensor')), may hold values from 0.25 to 1
- expert_ids: int32 [65536], P(('expert', 'tensor')), may hold values from 0 to 255, as said below
- slots: int32 [65536], P(('expert', 'tensor')), may hold values from -1 to 1, as said below
- w_in: bfloat16 [256, 768, 3072], P(('expert', 'tensor')), may hold values from -0.21875 to 0.21875
- w_out: bfloat16 [256, 768, 3072], P(('expert', 'tensor')), may hold values from -0.109375 to 0.109375
Outputs:
- mixed: bfloat16 [65536, 768], P(('expert', 'tensor'))
The draws below stay inside these ranges and needn't reach their ends.
Inputs may be any that keep to these rules, and one draw needn't show every extreme that they name: `expert_ids`: each token's expert, 0 to 255; in every block of 256 tokens one expert, the same in all blocks, is chosen by 2 + 1 or more tokens at positions that differ from block to block. `slots`: the slot of a token is the number of earlier tokens of its block of 256 that chose the same expert, if that is below 2, else -1; so at most 2 tokens of one block reach one expert, and one expert receives exactly 2 from every block.
All inputs are finite; a program needn't handle non-finite values.
Results may differ from the reference program's by a relative error of at most 0.0037.
Values may be sent and summed in bfloat16 or wider, within the bound.
A program may use at most 64 MiB of HBM per device.

```python
import jax
import jax.numpy as jnp
from jax import lax

D = 768
FF = 3072
TOK_DEV = 256
EXPERTS = 256
CAP = 2
TOKENS = 65536


def routing_pair(key):
    blocks = TOKENS // TOK_DEV
    first, second, third = jax.random.split(jax.random.fold_in(key, 7), 3)
    chosen = jax.random.randint(first, (blocks, TOK_DEV), 0, EXPERTS).astype(jnp.int32)
    popular = jax.random.randint(second, (), 0, EXPERTS).astype(jnp.int32)
    block_keys = jax.random.split(third, blocks)
    orders = jax.vmap(lambda k: jax.random.permutation(k, TOK_DEV))(block_keys)
    inverse = jnp.argsort(orders, axis=1, stable=True)
    forced = inverse < CAP + 1
    chosen = jnp.where(forced, popular, chosen).astype(jnp.int32)
    positions = jnp.arange(TOK_DEV, dtype=jnp.int32)
    earlier_than = positions[None, :] < positions[:, None]

    def ranks(block_ids):
        same = block_ids[:, None] == block_ids[None, :]
        count = jnp.sum((same & earlier_than).astype(jnp.int32), axis=1)
        return jnp.where(count < CAP, count, -1).astype(jnp.int32)
    slot_values = lax.map(ranks, chosen)
    return (chosen.reshape(TOKENS), slot_values.reshape(TOKENS))


def draw_expert_ids(key, part):
    return routing_pair(key)[0]


def draw_slots(key, part):
    return routing_pair(key)[1]


def level_of(key, shape, pieces, least, top_value):
    loudness = 1.0
    for axis_at, parts in pieces:
        heights = jax.random.uniform(jax.random.fold_in(jax.random.fold_in(key, 6), axis_at), (parts,), jnp.float32, least / len(pieces), top_value / len(pieces))
        loudness = loudness * jnp.repeat(jnp.exp(heights), shape[axis_at] // parts).reshape((-1,) + (1,) * (len(shape) - 1 - axis_at))
    return loudness


def noise(stream_key, dims, deviation, most, shards=(), kind=jnp.bfloat16):
    values = deviation * jax.random.normal(stream_key, dims, jnp.float32)
    if shards:
        values = values * level_of(stream_key, dims, shards, -0.22, 0.18)
    return jnp.clip(values, -most, most).astype(kind)


def setup_inputs(seed: int = 0) -> dict:
    key_list = jax.random.split(jax.random.key(seed), 8)
    tokens = noise(key_list[0], (TOKENS, D), 1.0, 6.0, ((0, 256),))
    norm_gain = jnp.clip(1.0 + 0.15 * jax.random.normal(key_list[1], (D,), jnp.float32), 0.25, 1.75)
    gates = jnp.clip(0.25 + 0.75 * jax.random.uniform(key_list[2], (TOKENS,), jnp.float32) ** level_of(key_list[2], (TOKENS,), ((0, 256),), -0.2, 0.2), 0.25, 1.0)
    expert_ids = draw_expert_ids(jax.random.fold_in(key_list[7], 71), 0)
    slots = draw_slots(jax.random.fold_in(key_list[7], 71), 0)
    w_in = noise(key_list[5], (EXPERTS, D, FF), D ** -0.5, 0.21875, ((0, 256),))
    w_out = noise(key_list[6], (EXPERTS, D, FF), FF ** -0.5, 0.109375, ((0, 256),))
    return {"tokens": tokens, "norm_gain": norm_gain, "gates": gates, "expert_ids": expert_ids, "slots": slots, "w_in": w_in, "w_out": w_out}


def slot_mask(expert_ids, slots):
    index = expert_ids * CAP + slots
    columns = jnp.arange(EXPERTS * CAP, dtype=jnp.int32)
    valid = slots >= 0
    return ((index[:, None] == columns[None, :]) & valid[:, None]).astype(jnp.bfloat16)

def normalize(tokens, norm_gain):
    values = tokens.astype(jnp.float32)
    square = lax.optimization_barrier(jnp.mean(values * values, axis=-1, keepdims=True))
    return (values * lax.rsqrt(square + 1e-06) * norm_gain[None, :]).astype(jnp.bfloat16)

def reference(tokens, norm_gain, gates, expert_ids, slots, w_in, w_out):
    blocks = TOKENS // TOK_DEV
    tok_blocks = tokens.reshape(blocks, TOK_DEV, D)
    id_blocks = expert_ids.reshape(blocks, TOK_DEV)
    slot_blocks = slots.reshape(blocks, TOK_DEV)
    gate_blocks = gates.reshape(blocks, TOK_DEV)

    def prepare(items):
        block_tok, block_ids, block_slots = items
        normed = normalize(block_tok, norm_gain)
        masked = slot_mask(block_ids, block_slots)
        filled = jnp.dot(masked.T, normed, preferred_element_type=jnp.float32)
        return filled.astype(jnp.bfloat16).reshape(EXPERTS, CAP, D)
    buffer = lax.map(prepare, (tok_blocks, id_blocks, slot_blocks))

    def run_expert(items):
        rows, weight_in, weight_out = items
        flat = rows.reshape(blocks * CAP, D)
        hidden = jnp.maximum(jnp.dot(flat, weight_in, preferred_element_type=jnp.float32), 0.0).astype(jnp.bfloat16)
        result = jnp.dot(hidden, weight_out.T, preferred_element_type=jnp.float32)
        return result.astype(jnp.bfloat16).reshape(blocks, CAP, D)
    expert_out = lax.map(run_expert, (jnp.transpose(buffer, (1, 0, 2, 3)), w_in, w_out))
    expert_out = jnp.transpose(expert_out, (1, 0, 2, 3))

    def finish(items):
        block_tok, block_ids, block_slots, block_gate, block_out = items
        masked = slot_mask(block_ids, block_slots)
        picked = jnp.dot(masked, block_out.reshape(EXPERTS * CAP, D), preferred_element_type=jnp.float32)
        return (block_tok.astype(jnp.float32) + block_gate[:, None] * picked).astype(jnp.bfloat16)
    mixed = lax.map(finish, (tok_blocks, id_blocks, slot_blocks, gate_blocks, expert_out))
    return mixed.reshape(TOKENS, D)
```

```python
import functools

import jax
import jax.numpy as jnp
from jax import lax
from jax.experimental import pallas as pl
from jax.experimental.pallas import tpu as pltpu
from jax.sharding import PartitionSpec as P

MESH = pl.DeviceIdType.MESH
NX, NY, NZ, NC = 4, 4, 8, 2
N = NX * NY * NZ * NC


def position():
    e, t = lax.axis_index("expert"), lax.axis_index("tensor")
    core, z, y, xh = lax.rem(e, NC), lax.rem(e // NC, NZ), lax.rem(e // (NC * NZ), NY), e // (NC * NZ * NY)
    return xh * 2 + t, y, z, core


def device_at(here, dx, dy, dz, dc):
    x, y, z, core = here
    x, y, z, core = lax.rem(x + dx, NX), lax.rem(y + dy, NY), lax.rem(z + dz, NZ), lax.rem(core + dc, NC)
    return ((x // 2 * NY + y) * NZ + z) * NC + core, lax.rem(x, 2)


def in_plane(i):
    return lax.rem(i, NX), i // (NX * NC), lax.rem(i // NX, NC)


def enter(here, met):
    barrier = pltpu.get_barrier_semaphore()
    plane = NX * NY * NC - 1

    def greet(i, _):
        dx, dy, dc = in_plane(i + 1)
        pl.semaphore_signal(barrier, inc=1, device_id=device_at(here, dx, dy, 0, dc), device_id_type=MESH)
        return 0

    lax.fori_loop(0, plane, greet, 0)
    for dz in range(1, NZ):
        pl.semaphore_signal(barrier, inc=1, device_id=device_at(here, 0, 0, dz, 0), device_id_type=MESH)
    pl.semaphore_wait(barrier, plane + NZ - 1)
    for dz in range(1, NZ):
        pl.semaphore_signal(met, inc=1, device_id=device_at(here, 0, 0, dz, 0), device_id_type=MESH)
    pl.semaphore_wait(met, NZ - 1)


def exchange_kernel(src, dst, met, send_sem, recv_sem):
    here = position()
    e, t = lax.axis_index("expert"), lax.axis_index("tensor")
    me = e * 2 + t
    enter(here, met)

    def send(i, _):
        i = i + 1
        dz = lax.rem(i, NZ)
        dx, dy, dc = in_plane(i // NZ)
        to = device_at(here, dx, dy, dz, dc)
        pltpu.make_async_remote_copy(
            src.at[to[0] * 2 + to[1]], dst.at[me], send_sem, recv_sem, device_id=to, device_id_type=MESH
        ).start()
        return 0

    lax.fori_loop(0, N - 1, send, 0)
    dst[me] = src[me]
    rest = pltpu.make_async_remote_copy(
        src.at[pl.ds(0, N - 1)], dst.at[pl.ds(0, N - 1)], send_sem, recv_sem,
        device_id=device_at(here, 0, 0, 0, 1), device_id_type=MESH,
    )
    rest.wait_send()
    rest.wait_recv()


def exchange(blocks):
    return pl.pallas_call(
        exchange_kernel,
        out_shape=jax.ShapeDtypeStruct(blocks.shape, blocks.dtype),
        in_specs=[pl.BlockSpec(memory_space=pltpu.VMEM)],
        out_specs=pl.BlockSpec(memory_space=pltpu.VMEM),
        scratch_shapes=[
            pltpu.SemaphoreType.REGULAR,
            pltpu.SemaphoreType.DMA,
            pltpu.SemaphoreType.DMA,
        ],
        compiler_params=pltpu.CompilerParams(collective_id=0, has_side_effects=True),
    )(blocks)


def slot_mask(expert_ids, slots, experts, capacity):
    index = expert_ids * capacity + slots
    columns = jnp.arange(experts * capacity, dtype=jnp.int32)
    valid = slots >= 0
    return ((index[:, None] == columns[None, :]) & valid[:, None]).astype(jnp.bfloat16)


def normalize(tokens, norm_gain):
    values = tokens.astype(jnp.float32)
    square = jnp.mean(values * values, axis=-1, keepdims=True)
    return (values * lax.rsqrt(square + 1e-06) * norm_gain[None, :]).astype(jnp.bfloat16)


def local(tokens, norm_gain, gates, expert_ids, slots, w_in, w_out):
    tok_dev, width = tokens.shape
    experts, capacity = N, 2
    normed = normalize(tokens, norm_gain)
    masked = slot_mask(expert_ids, slots, experts, capacity)
    buffer = jnp.dot(masked.T, normed, preferred_element_type=jnp.float32).astype(jnp.bfloat16)
    arrived = exchange(buffer.reshape(experts, capacity, width))
    rows = arrived.reshape(experts * capacity, width)
    hidden = jnp.maximum(jnp.dot(rows, w_in[0], preferred_element_type=jnp.float32), 0.0).astype(
        jnp.bfloat16
    )
    result = lax.dot_general(
        hidden, w_out[0], (((1,), (1,)), ((), ())), preferred_element_type=jnp.float32
    )
    returned = exchange(result.astype(jnp.bfloat16).reshape(experts, capacity, width))
    picked = jnp.dot(
        masked, returned.reshape(experts * capacity, width), preferred_element_type=jnp.float32
    )
    return (tokens.astype(jnp.float32) + gates[:, None] * picked).astype(jnp.bfloat16)


def solution(mesh):
    in_specs = (
        P(("expert", "tensor"), None),
        P(),
        P(("expert", "tensor")),
        P(("expert", "tensor")),
        P(("expert", "tensor")),
        P(("expert", "tensor"), None, None),
        P(("expert", "tensor"), None, None),
    )
    out_specs = P(("expert", "tensor"), None)
    return jax.shard_map(local, mesh=mesh, in_specs=in_specs, out_specs=out_specs, check_vma=False)
```

```python
import functools

import jax
import jax.numpy as jnp
from jax import lax
from jax.experimental import pallas as pl
from jax.experimental.pallas import tpu as pltpu
from jax.sharding import PartitionSpec as P

MESH = pl.DeviceIdType.MESH
NX, NY, NZ, NC = 4, 4, 8, 2
N = NX * NY * NZ * NC
LANES, ROWS = 128, 16
CHUNKS = ((0, 2), (1, 2))
PARTNERS = N // len(CHUNKS)
ALONG_Z = NZ // len(CHUNKS)
TILES = PARTNERS * 2 // ROWS


def position():
    e, t = lax.axis_index("expert"), lax.axis_index("tensor")
    core, z, y, xh = lax.rem(e, NC), lax.rem(e // NC, NZ), lax.rem(e // (NC * NZ), NY), e // (NC * NZ * NY)
    return xh * 2 + t, y, z, core


def device_at(here, dx, dy, dz, dc):
    x, y, z, core = here
    x, y, z, core = lax.rem(x + dx, NX), lax.rem(y + dy, NY), lax.rem(z + dz, NZ), lax.rem(core + dc, NC)
    return ((x // 2 * NY + y) * NZ + z) * NC + core, lax.rem(x, 2)


def in_plane(i):
    return lax.rem(i, NX), i // (NX * NC), lax.rem(i // NX, NC)


def partner(here, chunk, i, sign):
    first, step = CHUNKS[chunk]
    dz = lax.rem(first + step * lax.rem(i, ALONG_Z), NZ)
    dx, dy, dc = in_plane(i // ALONG_Z)
    if sign < 0:
        dx, dy, dz = NX - dx, NY - dy, NZ - dz
    return device_at(here, dx, dy, dz, dc)


def pair(ref, i):
    return ref.at[i // 8, :, pl.ds(2 * lax.rem(i, 8), 2), :]


def greet(here):
    barrier = pltpu.get_barrier_semaphore()

    def signal(i, _):
        dx, dy, dc = in_plane(i + 1)
        pl.semaphore_signal(barrier, inc=1, device_id=device_at(here, dx, dy, 0, dc), device_id_type=MESH)
        return 0

    lax.fori_loop(0, NX * NY * NC - 1, signal, 0)
    for dz in range(1, NZ):
        pl.semaphore_signal(barrier, inc=1, device_id=device_at(here, 0, 0, dz, 0), device_id_type=MESH)


def meet(here, met):
    pl.semaphore_wait(pltpu.get_barrier_semaphore(), NX * NY * NC + NZ - 2)
    for dz in range(1, NZ):
        pl.semaphore_signal(met, inc=1, device_id=device_at(here, 0, 0, dz, 0), device_id_type=MESH)
    pl.semaphore_wait(met, NZ - 1)


def columns(ref, tiles, count):
    return jnp.concatenate([ref[tiles, j].reshape(count * ROWS, LANES) for j in range(ref.shape[1])], axis=1)


def kernel(tokens, gain, gates, ids, slots, w_in, w_out, mixed,
           outbox, inbox, results, returned, w1, w2, hidden,
           met, w_sem, out_sem, in_sem, back_sem, home_sem):
    here = position()
    me = lax.axis_index("expert") * 2 + lax.axis_index("tensor")
    n_tok, width = tokens.shape
    parts = width // LANES
    load1 = pltpu.make_async_copy(w_in.at[0], w1, w_sem.at[0])
    load2 = pltpu.make_async_copy(w_out.at[0], w2, w_sem.at[1])
    greet(here)
    load1.start()
    load2.start()

    values = tokens[...].astype(jnp.float32)
    square = jnp.mean(values * values, axis=-1, keepdims=True)
    normed = (values * lax.rsqrt(square + 1e-06) * gain[...]).astype(jnp.bfloat16)
    index = jnp.where(slots[...] >= 0, ids[...] * 2 + slots[...], -1)
    picks = (lax.broadcasted_iota(jnp.int32, (2 * N, n_tok), 0) == index).astype(jnp.bfloat16)
    for j in range(parts // 2):
        block = jnp.dot(picks, normed[:, j * 256 : j * 256 + 256], preferred_element_type=jnp.float32).astype(jnp.bfloat16)
        for half in range(2):
            outbox[:, 2 * j + half] = block[:, half * LANES : (half + 1) * LANES].reshape(2 * N // ROWS, ROWS, LANES)
    meet(here, met)

    def post(chunk, first):
        def send(i, _):
            to = partner(here, chunk, i, 1)
            pltpu.make_async_remote_copy(
                pair(outbox, to[0] * 2 + to[1]), pair(inbox, chunk * PARTNERS + i), out_sem, in_sem.at[chunk],
                device_id=to, device_id_type=MESH,
            ).start()
            return 0

        lax.fori_loop(first, PARTNERS, send, 0)

    post(0, 1)
    own = pltpu.make_async_copy(pair(outbox, me), pair(inbox, 0), in_sem.at[0])
    own.start()
    for chunk in range(1, len(CHUNKS)):
        post(chunk, 0)
    load1.wait()
    load2.wait()

    near = device_at(here, 0, 0, 0, 1)
    for chunk in range(len(CHUNKS)):
        tiles = pl.ds(chunk * TILES, TILES)
        pltpu.make_async_remote_copy(
            inbox.at[tiles], inbox.at[tiles], out_sem, in_sem.at[chunk], device_id=near, device_id_type=MESH
        ).wait_recv()
        rows = columns(inbox, tiles, TILES)

        def widen(k, _):
            at = pl.ds(pl.multiple_of(k * 256, 256), 256)
            h = jnp.dot(rows, w1[:, at], preferred_element_type=jnp.float32)
            hidden[:, at] = jnp.maximum(h, 0.0).astype(jnp.bfloat16)
            return 0

        lax.fori_loop(0, w1.shape[1] // 256, widen, 0)
        for j in range(parts // 2):
            r = lax.dot_general(
                hidden[...], w2[j * 256 : j * 256 + 256, :], (((1,), (1,)), ((), ())), preferred_element_type=jnp.float32
            ).astype(jnp.bfloat16)
            for half in range(2):
                results[tiles, 2 * j + half] = r[:, half * LANES : (half + 1) * LANES].reshape(TILES, ROWS, LANES)

        def reply(i, _):
            to = partner(here, chunk, i, -1)
            pltpu.make_async_remote_copy(
                pair(results, chunk * PARTNERS + i), pair(returned, me), back_sem, home_sem,
                device_id=to, device_id_type=MESH,
            ).start()
            return 0

        lax.fori_loop(1 if chunk == 0 else 0, PARTNERS, reply, 0)
        if chunk == 0:
            pltpu.make_async_copy(pair(results, 0), pair(returned, me), home_sem).start()

    everything = pltpu.make_async_remote_copy(returned, returned, back_sem, home_sem, device_id=near, device_id_type=MESH)
    everything.wait_recv()
    rest = columns(returned, slice(None), 2 * N // ROWS)
    picked = lax.dot_general(picks, rest, (((0,), (0,)), ((), ())), preferred_element_type=jnp.float32)
    weight = jnp.transpose(jnp.broadcast_to(gates[...], (LANES, n_tok)))
    weight = jnp.concatenate([weight] * parts, axis=1)
    mixed[...] = (tokens[...].astype(jnp.float32) + weight * picked).astype(jnp.bfloat16)
    left = 2 * N // ROWS - 1
    for box, sem in ((outbox, out_sem), (results, back_sem)):
        pltpu.make_async_copy(box.at[pl.ds(0, left)], box.at[pl.ds(0, left)], sem).wait()
        pltpu.make_async_copy(box.at[0, :, pl.ds(0, ROWS - 2), :], box.at[0, :, pl.ds(0, ROWS - 2), :], sem).wait()


def local(tokens, norm_gain, gates, expert_ids, slots, w_in, w_out):
    n_tok, width = tokens.shape
    hidden = w_in.shape[2]
    box = pltpu.VMEM((2 * N // ROWS, width // LANES, ROWS, LANES), jnp.bfloat16)
    vmem, anywhere = pl.BlockSpec(memory_space=pltpu.VMEM), pl.BlockSpec(memory_space=pl.ANY)
    return pl.pallas_call(
        kernel,
        out_shape=jax.ShapeDtypeStruct(tokens.shape, tokens.dtype),
        in_specs=[vmem] * 5 + [anywhere] * 2,
        out_specs=vmem,
        scratch_shapes=[
            box, box, box, box,
            pltpu.VMEM((width, hidden), jnp.bfloat16),
            pltpu.VMEM((width, hidden), jnp.bfloat16),
            pltpu.VMEM((PARTNERS * 2, hidden), jnp.bfloat16),
            pltpu.SemaphoreType.REGULAR,
            pltpu.SemaphoreType.DMA((2,)),
            pltpu.SemaphoreType.DMA,
            pltpu.SemaphoreType.DMA((len(CHUNKS),)),
            pltpu.SemaphoreType.DMA,
            pltpu.SemaphoreType.DMA,
        ],
        compiler_params=pltpu.CompilerParams(collective_id=0, has_side_effects=True),
    )(tokens, norm_gain.reshape(1, width), gates.reshape(1, n_tok), expert_ids.reshape(1, n_tok),
      slots.reshape(1, n_tok), w_in, w_out)


def solution(mesh):
    in_specs = (
        P(("expert", "tensor"), None),
        P(),
        P(("expert", "tensor")),
        P(("expert", "tensor")),
        P(("expert", "tensor")),
        P(("expert", "tensor"), None, None),
        P(("expert", "tensor"), None, None),
    )
    out_specs = P(("expert", "tensor"), None)
    return jax.shard_map(local, mesh=mesh, in_specs=in_specs, out_specs=out_specs, check_vma=False)
```

```python
import functools

import jax
import jax.numpy as jnp
from jax import lax
from jax.experimental import pallas as pl
from jax.experimental.pallas import tpu as pltpu
from jax.sharding import PartitionSpec as P

LOGICAL = pl.DeviceIdType.LOGICAL
NX, NY, NZ, NC = 4, 4, 8, 2
N = NX * NY * NZ * NC
LANES, ROWS = 128, 16
CHUNKS = ((0, 2), (1, 2))
PARTNERS = N // len(CHUNKS)
ALONG_Z = NZ // len(CHUNKS)
TILES = PARTNERS * 2 // ROWS
PLANE = [(dc, dx) for dc in range(NC) for dx in range(NX)]


class Place:
    def __init__(self):
        e, t = lax.axis_index("expert"), lax.axis_index("tensor")
        core, z = lax.rem(e, NC), lax.rem(e // NC, NZ)
        y, xh = lax.rem(e // (NC * NZ), NY), e // (NC * NZ * NY)
        self.me = e * 2 + t
        self.y = y
        xs = [lax.rem(xh * 2 + t + d, NX) for d in range(NX)]
        zs = [lax.rem(z + d, NZ) for d in range(NZ)]
        cs = [lax.rem(core + d, NC) for d in range(NC)]
        self.along_x = [(x // 2 * 128 + lax.rem(x, 2), x // 2 * 16, lax.rem(x, 2)) for x in xs]
        self.along_z = [(z * 4, z // 2, lax.rem(z, 2) * 4) for z in zs]
        self.along_c = [(c * 2, c * 2) for c in cs]

    def row(self, dy):
        y = lax.rem(self.y + dy, NY)
        return y * 32, y * 4

    def at(self, row, dx, dz, dc):
        x, z, c = self.along_x[dx], self.along_z[dz], self.along_c[dc]
        return row[0] + z[0] + (x[0] + c[0]), row[1] + z[1] + x[1], z[2] + (x[2] + c[1])


def pair(ref, tile, i):
    return ref.at[tile, :, pl.ds(2 * i, 2), :]


def greet(place):
    barrier = pltpu.get_barrier_semaphore()
    rows = [place.row(dy) for dy in range(NY)]
    for dz in range(1, NZ):
        pl.semaphore_signal(barrier, inc=1, device_id=place.at(rows[0], 0, dz, 0)[0], device_id_type=LOGICAL)
    for dy in range(NY):
        for dc, dx in PLANE:
            if dy or dc or dx:
                pl.semaphore_signal(barrier, inc=1, device_id=place.at(rows[dy], dx, 0, dc)[0], device_id_type=LOGICAL)


def columns(ref, tiles, count):
    return jnp.concatenate([ref[tiles, j].reshape(count * ROWS, LANES) for j in range(ref.shape[1])], axis=1)


def kernel(tokens_hbm, gain_hbm, gates_hbm, ids_hbm, slots_hbm, w_in, w_out, mixed,
           tokens, gain, gates, ids, slots, outbox, inbox, results, returned, w1, w2, hidden,
           met, arg_sem, w_sem, out_sem, in_sem, back_sem, home_sem):
    loads = [
        pltpu.make_async_copy(hbm, vmem, arg_sem.at[i])
        for i, (hbm, vmem) in enumerate(
            ((tokens_hbm, tokens), (gain_hbm, gain), (gates_hbm, gates), (ids_hbm, ids), (slots_hbm, slots))
        )
    ]
    for load in loads:
        load.start()
    place = Place()
    me = place.me
    n_tok, width = tokens.shape
    parts = width // LANES
    load1 = pltpu.make_async_copy(w_in.at[0], w1, w_sem.at[0])
    load2 = pltpu.make_async_copy(w_out.at[0], w2, w_sem.at[1])
    greet(place)
    for load in loads:
        load.wait()
    load1.start()
    load2.start()

    values = tokens[...].astype(jnp.float32)
    square = jnp.mean(values * values, axis=-1, keepdims=True)
    normed = (values * lax.rsqrt(square + 1e-06) * gain[...].reshape(1, width)).astype(jnp.bfloat16)
    index = jnp.where(slots[...] >= 0, ids[...] * 2 + slots[...], -1)
    picks = (lax.broadcasted_iota(jnp.int32, (2 * N, n_tok), 0) == index).astype(jnp.bfloat16)
    for j in range(parts // 2):
        block = jnp.dot(picks, normed[:, j * 256 : j * 256 + 256], preferred_element_type=jnp.float32).astype(jnp.bfloat16)
        for half in range(2):
            outbox[:, 2 * j + half] = block[:, half * LANES : (half + 1) * LANES].reshape(2 * N // ROWS, ROWS, LANES)

    here = place.row(0)

    def post(chunk, dy, row, combos):
        first, step = CHUNKS[chunk]
        for a, dc, dx in combos:
            number, tile, i = place.at(row, dx, first + step * a, dc)
            pltpu.make_async_remote_copy(
                pair(outbox, tile, i), pair(inbox, chunk * TILES + dy * ALONG_Z + a, dc * NX + dx),
                out_sem, in_sem.at[chunk], device_id=number, device_id_type=LOGICAL,
            ).start()

    pl.semaphore_wait(pltpu.get_barrier_semaphore(), NX * NY * NC + NZ - 2)
    for dz in range(1, NZ):
        pl.semaphore_signal(met, inc=1, device_id=place.at(here, 0, dz, 0)[0], device_id_type=LOGICAL)
    for chunk in range(len(CHUNKS)):
        post(chunk, 0, here, [(a, 0, 0) for a in range(1 if chunk == 0 else 0, ALONG_Z)])
    post(0, 0, here, [(0, dc, dx) for dc, dx in PLANE if dc or dx])

    def post_row(dy, _):
        post(0, dy, place.row(dy), [(0, dc, dx) for dc, dx in PLANE])
        return 0

    lax.fori_loop(1, NY, post_row, 0)
    own = pltpu.make_async_copy(pair(outbox, me // 8, lax.rem(me, 8)), pair(inbox, 0, 0), in_sem.at[0])
    own.start()
    pl.semaphore_wait(met, NZ - 1)
    for chunk in range(len(CHUNKS)):
        steps = range(1 if chunk == 0 else 0, ALONG_Z)
        post(chunk, 0, here, [(a, dc, dx) for dc, dx in PLANE for a in steps if dc or dx])

        def post_rest(dy, _):
            post(chunk, dy, place.row(dy), [(a, dc, dx) for dc, dx in PLANE for a in steps])
            return 0

        lax.fori_loop(1, NY, post_rest, 0)
    load1.wait()
    load2.wait()

    near = place.at(here, 0, 0, 1)[0]
    for chunk in range(len(CHUNKS)):
        tiles = pl.ds(chunk * TILES, TILES)
        pltpu.make_async_remote_copy(
            inbox.at[tiles], inbox.at[tiles], out_sem, in_sem.at[chunk], device_id=near, device_id_type=LOGICAL
        ).wait_recv()
        rows = columns(inbox, tiles, TILES)

        def widen(k, _):
            at = pl.ds(pl.multiple_of(k * 256, 256), 256)
            h = jnp.dot(rows, w1[:, at], preferred_element_type=jnp.float32)
            hidden[:, at] = jnp.maximum(h, 0.0).astype(jnp.bfloat16)
            return 0

        lax.fori_loop(0, w1.shape[1] // 256, widen, 0)
        for j in range(parts // 2):
            r = lax.dot_general(
                hidden[...], w2[j * 256 : j * 256 + 256, :], (((1,), (1,)), ((), ())), preferred_element_type=jnp.float32
            ).astype(jnp.bfloat16)
            for half in range(2):
                results[tiles, 2 * j + half] = r[:, half * LANES : (half + 1) * LANES].reshape(TILES, ROWS, LANES)

        home = pair(returned, me // 8, lax.rem(me, 8))

        def reply(dy, row, combos):
            first, step = CHUNKS[chunk]
            for a, dc, dx in combos:
                number = place.at(row, -dx % NX, -(first + step * a) % NZ, dc)[0]
                pltpu.make_async_remote_copy(
                    pair(results, chunk * TILES + dy * ALONG_Z + a, dc * NX + dx), home,
                    back_sem, home_sem, device_id=number, device_id_type=LOGICAL,
                ).start()

        def reply_row(dy, _):
            reply(dy, place.row(NY - dy), [(a, dc, dx) for dc, dx in PLANE for a in range(ALONG_Z)])
            return 0

        reply(0, here, [(a, dc, dx) for dc, dx in PLANE for a in range(ALONG_Z) if chunk or a or dc or dx])
        lax.fori_loop(1, NY, reply_row, 0)
        if chunk == 0:
            pltpu.make_async_copy(pair(results, 0, 0), home, home_sem).start()

    everything = pltpu.make_async_remote_copy(returned, returned, back_sem, home_sem, device_id=near, device_id_type=LOGICAL)
    everything.wait_recv()
    rest = columns(returned, slice(None), 2 * N // ROWS)
    picked = lax.dot_general(picks, rest, (((0,), (0,)), ((), ())), preferred_element_type=jnp.float32)
    weight = jnp.transpose(jnp.broadcast_to(gates[...], (LANES, n_tok)))
    weight = jnp.concatenate([weight] * parts, axis=1)
    mixed[...] = (tokens[...].astype(jnp.float32) + weight * picked).astype(jnp.bfloat16)
    left = 2 * N // ROWS - 1
    for box, sem in ((outbox, out_sem), (results, back_sem)):
        pltpu.make_async_copy(box.at[pl.ds(0, left)], box.at[pl.ds(0, left)], sem).wait()
        pltpu.make_async_copy(box.at[0, :, pl.ds(0, ROWS - 2), :], box.at[0, :, pl.ds(0, ROWS - 2), :], sem).wait()


def local(tokens, norm_gain, gates, expert_ids, slots, w_in, w_out):
    n_tok, width = tokens.shape
    hidden = w_in.shape[2]
    box = pltpu.VMEM((2 * N // ROWS, width // LANES, ROWS, LANES), jnp.bfloat16)
    vmem, anywhere = pl.BlockSpec(memory_space=pltpu.VMEM), pl.BlockSpec(memory_space=pl.ANY)
    return pl.pallas_call(
        kernel,
        out_shape=jax.ShapeDtypeStruct(tokens.shape, tokens.dtype),
        in_specs=[anywhere] * 7,
        out_specs=vmem,
        scratch_shapes=[
            pltpu.VMEM((n_tok, width), tokens.dtype),
            pltpu.VMEM((width,), jnp.float32),
            pltpu.VMEM((1, n_tok), jnp.float32),
            pltpu.VMEM((1, n_tok), jnp.int32),
            pltpu.VMEM((1, n_tok), jnp.int32),
            box, box, box, box,
            pltpu.VMEM((width, hidden), jnp.bfloat16),
            pltpu.VMEM((width, hidden), jnp.bfloat16),
            pltpu.VMEM((PARTNERS * 2, hidden), jnp.bfloat16),
            pltpu.SemaphoreType.REGULAR,
            pltpu.SemaphoreType.DMA((5,)),
            pltpu.SemaphoreType.DMA((2,)),
            pltpu.SemaphoreType.DMA,
            pltpu.SemaphoreType.DMA((len(CHUNKS),)),
            pltpu.SemaphoreType.DMA,
            pltpu.SemaphoreType.DMA,
        ],
        compiler_params=pltpu.CompilerParams(collective_id=0, has_side_effects=True),
    )(tokens, norm_gain, gates.reshape(1, n_tok), expert_ids.reshape(1, n_tok),
      slots.reshape(1, n_tok), w_in, w_out)


def solution(mesh):
    in_specs = (
        P(("expert", "tensor"), None),
        P(),
        P(("expert", "tensor")),
        P(("expert", "tensor")),
        P(("expert", "tensor")),
        P(("expert", "tensor"), None, None),
        P(("expert", "tensor"), None, None),
    )
    out_specs = P(("expert", "tensor"), None)
    return jax.shard_map(local, mesh=mesh, in_specs=in_specs, out_specs=out_specs, check_vma=False)
```

```python
import functools

import jax
import jax.numpy as jnp
from jax import lax
from jax.experimental import pallas as pl
from jax.experimental.pallas import tpu as pltpu
from jax.sharding import PartitionSpec as P

LOGICAL = pl.DeviceIdType.LOGICAL
NX, NY, NZ, NC = 4, 4, 8, 2
N = NX * NY * NZ * NC
LANES, ROWS = 128, 16
VMEM_LIMIT = 24 * 1024 * 1024
CHUNKS = ((0, 2), (1, 2))
PARTNERS = N // len(CHUNKS)
ALONG_Z = NZ // len(CHUNKS)
TILES = PARTNERS * 2 // ROWS
GROUPS = ((0, (1, 3)), (0, (2,)), (1, (0, 3)), (1, (1, 2)))
PLANE = [(dc, dx) for dc in range(NC) for dx in range(NX)]


class Place:
    def __init__(self):
        e, t = lax.axis_index("expert"), lax.axis_index("tensor")
        core, z = lax.rem(e, NC), lax.rem(e // NC, NZ)
        y, xh = lax.rem(e // (NC * NZ), NY), e // (NC * NZ * NY)
        self.me = e * 2 + t
        self.y = y
        xs = [lax.rem(xh * 2 + t + d, NX) for d in range(NX)]
        zs = [lax.rem(z + d, NZ) for d in range(NZ)]
        cs = [lax.rem(core + d, NC) for d in range(NC)]
        self.along_x = [(x // 2 * 128 + lax.rem(x, 2), x // 2 * 16, lax.rem(x, 2)) for x in xs]
        self.along_z = [(z * 4, z // 2, lax.rem(z, 2) * 4) for z in zs]
        self.along_c = [(c * 2, c * 2) for c in cs]

    def row(self, dy):
        y = lax.rem(self.y + dy, NY)
        return y * 32, y * 4

    def at(self, row, dx, dz, dc):
        x, z, c = self.along_x[dx], self.along_z[dz], self.along_c[dc]
        return row[0] + z[0] + (x[0] + c[0]), row[1] + z[1] + x[1], z[2] + (x[2] + c[1])


def pair(ref, tile, i):
    return ref.at[tile, :, pl.ds(2 * i, 2), :]


def greet(place):
    barrier = pltpu.get_barrier_semaphore()
    rows = [place.row(dy) for dy in range(NY)]
    for dz in range(1, NZ):
        pl.semaphore_signal(barrier, inc=1, device_id=place.at(rows[0], 0, dz, 0)[0], device_id_type=LOGICAL)
    for dy in range(NY):
        for dc, dx in PLANE:
            if dy or dc or dx:
                pl.semaphore_signal(barrier, inc=1, device_id=place.at(rows[dy], dx, 0, dc)[0], device_id_type=LOGICAL)


def columns(ref, tiles, count):
    return jnp.concatenate([ref[tiles, j].reshape(count * ROWS, LANES) for j in range(ref.shape[1])], axis=1)


def kernel(tokens_hbm, gain_hbm, gates_hbm, ids_hbm, slots_hbm, w_in, w_out, gated,
           tokens, gain, gates, ids, slots, outbox, inbox, results, returned, w1, w2, hidden,
           met, arg_sem, w_sem, out_sem, in_sem, back_sem, home_sem):
    loads = [
        pltpu.make_async_copy(hbm, vmem, arg_sem.at[i])
        for i, (hbm, vmem) in enumerate(
            ((tokens_hbm, tokens), (gain_hbm, gain), (gates_hbm, gates), (ids_hbm, ids), (slots_hbm, slots))
        )
    ]
    for load in loads:
        load.start()
    place = Place()
    me = place.me
    n_tok, width = tokens.shape
    parts = width // LANES
    load1 = pltpu.make_async_copy(w_in.at[0], w1, w_sem.at[0])
    load2 = pltpu.make_async_copy(w_out.at[0], w2, w_sem.at[1])
    greet(place)
    for load in loads:
        load.wait()
    load1.start()
    load2.start()

    values = tokens[...].astype(jnp.float32)
    square = jnp.mean(values * values, axis=-1, keepdims=True)
    normed = (values * lax.rsqrt(square + 1e-06) * gain[...].reshape(1, width)).astype(jnp.bfloat16)
    index = jnp.where(slots[...] >= 0, ids[...] * 2 + slots[...], -1)
    picks = (lax.broadcasted_iota(jnp.int32, (2 * N, n_tok), 0) == index).astype(jnp.bfloat16)
    for j in range(parts // 2):
        block = jnp.dot(picks, normed[:, j * 256 : j * 256 + 256], preferred_element_type=jnp.float32).astype(jnp.bfloat16)
        for half in range(2):
            outbox[:, 2 * j + half] = block[:, half * LANES : (half + 1) * LANES].reshape(2 * N // ROWS, ROWS, LANES)

    here = place.row(0)

    def post(chunk, dy, row, combos):
        first, step = CHUNKS[chunk]
        for a, dc, dx in combos:
            number, tile, i = place.at(row, dx, first + step * a, dc)
            pltpu.make_async_remote_copy(
                pair(outbox, tile, i), pair(inbox, chunk * TILES + dy * ALONG_Z + a, dc * NX + dx),
                out_sem, in_sem.at[chunk], device_id=number, device_id_type=LOGICAL,
            ).start()

    pl.semaphore_wait(pltpu.get_barrier_semaphore(), NX * NY * NC + NZ - 2)
    for dz in range(1, NZ):
        pl.semaphore_signal(met.at[NZ - dz], inc=1, device_id=place.at(here, 0, dz, 0)[0], device_id_type=LOGICAL)
    for chunk in range(len(CHUNKS)):
        post(chunk, 0, here, [(a, 0, 0) for a in range(1 if chunk == 0 else 0, ALONG_Z)])
    post(0, 0, here, [(0, dc, dx) for dc, dx in PLANE if dc or dx])

    def post_row(dy, _):
        post(0, dy, place.row(dy), [(0, dc, dx) for dc, dx in PLANE])
        return 0

    lax.fori_loop(1, NY, post_row, 0)
    own = pltpu.make_async_copy(pair(outbox, me // 8, lax.rem(me, 8)), pair(inbox, 0, 0), in_sem.at[0])
    own.start()
    for chunk, group in GROUPS:
        first, step = CHUNKS[chunk]
        for a in group:
            pl.semaphore_wait(met.at[first + step * a], 1)
        post(chunk, 0, here, [(a, dc, dx) for dc, dx in PLANE for a in group if dc or dx])

        def post_rest(dy, _):
            post(chunk, dy, place.row(dy), [(a, dc, dx) for dc, dx in PLANE for a in group])
            return 0

        lax.fori_loop(1, NY, post_rest, 0)
    load1.wait()
    load2.wait()

    near = place.at(here, 0, 0, 1)[0]
    for chunk in range(len(CHUNKS)):
        tiles = pl.ds(chunk * TILES, TILES)
        pltpu.make_async_remote_copy(
            inbox.at[tiles], inbox.at[tiles], out_sem, in_sem.at[chunk], device_id=near, device_id_type=LOGICAL
        ).wait_recv()
        rows = columns(inbox, tiles, TILES)

        def widen(k, _):
            at = pl.ds(pl.multiple_of(k * 256, 256), 256)
            h = jnp.dot(rows, w1[:, at], preferred_element_type=jnp.float32)
            hidden[:, at] = jnp.maximum(h, 0.0).astype(jnp.bfloat16)
            return 0

        lax.fori_loop(0, w1.shape[1] // 256, widen, 0)
        for j in range(parts // 2):
            r = lax.dot_general(
                hidden[...], w2[j * 256 : j * 256 + 256, :], (((1,), (1,)), ((), ())), preferred_element_type=jnp.float32
            ).astype(jnp.bfloat16)
            for half in range(2):
                results[tiles, 2 * j + half] = r[:, half * LANES : (half + 1) * LANES].reshape(TILES, ROWS, LANES)

        home = pair(returned, me // 8, lax.rem(me, 8))

        def reply(dy, row, combos):
            first, step = CHUNKS[chunk]
            for a, dc, dx in combos:
                number = place.at(row, -dx % NX, -(first + step * a) % NZ, dc)[0]
                pltpu.make_async_remote_copy(
                    pair(results, chunk * TILES + dy * ALONG_Z + a, dc * NX + dx), home,
                    back_sem, home_sem, device_id=number, device_id_type=LOGICAL,
                ).start()

        def reply_row(dy, _):
            reply(dy, place.row(NY - dy), [(a, dc, dx) for dc, dx in PLANE for a in range(ALONG_Z)])
            return 0

        reply(0, here, [(a, dc, dx) for dc, dx in PLANE for a in range(ALONG_Z) if chunk or a or dc or dx])
        lax.fori_loop(1, NY, reply_row, 0)
        if chunk == 0:
            pltpu.make_async_copy(pair(results, 0, 0), home, home_sem).start()

    everything = pltpu.make_async_remote_copy(returned, returned, back_sem, home_sem, device_id=near, device_id_type=LOGICAL)
    everything.wait_recv()
    rest = columns(returned, slice(None), 2 * N // ROWS)
    picked = lax.dot_general(picks, rest, (((0,), (0,)), ((), ())), preferred_element_type=jnp.float32)
    weight = jnp.transpose(jnp.broadcast_to(gates[...], (LANES, n_tok)))
    weight = jnp.concatenate([weight] * parts, axis=1)
    gated[...] = weight * picked
    left = 2 * N // ROWS - 1
    for box, sem in ((outbox, out_sem), (results, back_sem)):
        pltpu.make_async_copy(box.at[pl.ds(0, left)], box.at[pl.ds(0, left)], sem).wait()
        pltpu.make_async_copy(box.at[0, :, pl.ds(0, ROWS - 2), :], box.at[0, :, pl.ds(0, ROWS - 2), :], sem).wait()


def local(tokens, norm_gain, gates, expert_ids, slots, w_in, w_out):
    n_tok, width = tokens.shape
    hidden = w_in.shape[2]
    box = pltpu.VMEM((2 * N // ROWS, width // LANES, ROWS, LANES), jnp.bfloat16)
    vmem, hbm = pl.BlockSpec(memory_space=pltpu.VMEM), pl.BlockSpec(memory_space=pltpu.HBM)
    gated = pl.pallas_call(
        kernel,
        out_shape=jax.ShapeDtypeStruct(tokens.shape, jnp.float32),
        in_specs=[hbm] * 7,
        out_specs=vmem,
        scratch_shapes=[
            pltpu.VMEM((n_tok, width), tokens.dtype),
            pltpu.VMEM((width,), jnp.float32),
            pltpu.VMEM((1, n_tok), jnp.float32),
            pltpu.VMEM((1, n_tok), jnp.int32),
            pltpu.VMEM((1, n_tok), jnp.int32),
            box, box, box, box,
            pltpu.VMEM((width, hidden), jnp.bfloat16),
            pltpu.VMEM((width, hidden), jnp.bfloat16),
            pltpu.VMEM((PARTNERS * 2, hidden), jnp.bfloat16),
            pltpu.SemaphoreType.REGULAR((NZ,)),
            pltpu.SemaphoreType.DMA((5,)),
            pltpu.SemaphoreType.DMA((2,)),
            pltpu.SemaphoreType.DMA,
            pltpu.SemaphoreType.DMA((len(CHUNKS),)),
            pltpu.SemaphoreType.DMA,
            pltpu.SemaphoreType.DMA,
        ],
        compiler_params=pltpu.CompilerParams(collective_id=0, has_side_effects=True, vmem_limit_bytes=VMEM_LIMIT),
    )(*[pltpu.with_memory_space_constraint(v, pltpu.HBM) for v in (tokens, norm_gain, gates.reshape(1, n_tok), expert_ids.reshape(1, n_tok),
      slots.reshape(1, n_tok), w_in, w_out)])
    return (tokens.astype(jnp.float32) + gated).astype(tokens.dtype)


def solution(mesh):
    in_specs = (
        P(("expert", "tensor"), None),
        P(),
        P(("expert", "tensor")),
        P(("expert", "tensor")),
        P(("expert", "tensor")),
        P(("expert", "tensor"), None, None),
        P(("expert", "tensor"), None, None),
    )
    out_specs = P(("expert", "tensor"), None)
    return jax.shard_map(local, mesh=mesh, in_specs=in_specs, out_specs=out_specs, check_vma=False)
```

```python
import functools

import jax
import jax.numpy as jnp
from jax import lax
from jax.experimental import pallas as pl
from jax.experimental.pallas import tpu as pltpu
from jax.sharding import PartitionSpec as P

LOGICAL = pl.DeviceIdType.LOGICAL
NX, NY, NZ, NC = 4, 4, 8, 2
N = NX * NY * NZ * NC
LANES, ROWS = 128, 16
VMEM_LIMIT = 24 * 1024 * 1024
CHUNKS = ((0, 3, 5), (4, 1, 7), (2, 6))
PLANE_TILES = NX * NY * NC * 2 // ROWS
GROUPS = ((0, (1,)), (0, (2,)), (1, (1,)), (1, (2,)), (1, (0,)), (2, (0,)), (2, (1,)))
PLANE = [(dc, dx) for dc in range(NC) for dx in range(NX)]


def first_tile(chunk):
    return sum(map(len, CHUNKS[:chunk])) * PLANE_TILES


class Place:
    def __init__(self):
        e, t = lax.axis_index("expert"), lax.axis_index("tensor")
        core, z = lax.rem(e, NC), lax.rem(e // NC, NZ)
        y, xh = lax.rem(e // (NC * NZ), NY), e // (NC * NZ * NY)
        self.me = e * 2 + t
        self.y = y
        xs = [lax.rem(xh * 2 + t + d, NX) for d in range(NX)]
        zs = [lax.rem(z + d, NZ) for d in range(NZ)]
        cs = [lax.rem(core + d, NC) for d in range(NC)]
        self.along_x = [(x // 2 * 128 + lax.rem(x, 2), x // 2 * 16, lax.rem(x, 2)) for x in xs]
        self.along_z = [(z * 4, z // 2, lax.rem(z, 2) * 4) for z in zs]
        self.along_c = [(c * 2, c * 2) for c in cs]

    def row(self, dy):
        y = lax.rem(self.y + dy, NY)
        return y * 32, y * 4

    def at(self, row, dx, dz, dc):
        x, z, c = self.along_x[dx], self.along_z[dz], self.along_c[dc]
        return row[0] + z[0] + (x[0] + c[0]), row[1] + z[1] + x[1], z[2] + (x[2] + c[1])


def pair(ref, tile, i):
    return ref.at[tile, :, pl.ds(2 * i, 2), :]


def greet(place):
    barrier = pltpu.get_barrier_semaphore()
    rows = [place.row(dy) for dy in range(NY)]
    for dz in range(1, NZ):
        pl.semaphore_signal(barrier, inc=1, device_id=place.at(rows[0], 0, dz, 0)[0], device_id_type=LOGICAL)
    for dy in range(NY):
        for dc, dx in PLANE:
            if dy or dc or dx:
                pl.semaphore_signal(barrier, inc=1, device_id=place.at(rows[dy], dx, 0, dc)[0], device_id_type=LOGICAL)


def columns(ref, tiles, count):
    return jnp.concatenate([ref[tiles, j].reshape(count * ROWS, LANES) for j in range(ref.shape[1])], axis=1)


def kernel(tokens_hbm, gain_hbm, gates_hbm, ids_hbm, slots_hbm, w_in, w_out, gated,
           tokens, gain, gates, ids, slots, outbox, inbox, results, returned, w1, w2, hidden,
           met, arg_sem, w_sem, out_sem, in_sem, back_sem, home_sem):
    loads = [
        pltpu.make_async_copy(hbm, vmem, arg_sem.at[i])
        for i, (hbm, vmem) in enumerate(
            ((tokens_hbm, tokens), (gain_hbm, gain), (gates_hbm, gates), (ids_hbm, ids), (slots_hbm, slots))
        )
    ]
    for load in loads:
        load.start()
    place = Place()
    me = place.me
    n_tok, width = tokens.shape
    parts = width // LANES
    load1 = pltpu.make_async_copy(w_in.at[0], w1, w_sem.at[0])
    load2 = pltpu.make_async_copy(w_out.at[0], w2, w_sem.at[1])
    greet(place)
    for load in loads:
        load.wait()
    load1.start()
    load2.start()

    values = tokens[...].astype(jnp.float32)
    square = jnp.mean(values * values, axis=-1, keepdims=True)
    normed = (values * lax.rsqrt(square + 1e-06) * gain[...].reshape(1, width)).astype(jnp.bfloat16)
    index = jnp.where(slots[...] >= 0, ids[...] * 2 + slots[...], -1)
    picks = (lax.broadcasted_iota(jnp.int32, (2 * N, n_tok), 0) == index).astype(jnp.bfloat16)
    for j in range(parts // 2):
        block = jnp.dot(picks, normed[:, j * 256 : j * 256 + 256], preferred_element_type=jnp.float32).astype(jnp.bfloat16)
        for half in range(2):
            outbox[:, 2 * j + half] = block[:, half * LANES : (half + 1) * LANES].reshape(2 * N // ROWS, ROWS, LANES)

    here = place.row(0)

    def post(chunk, dy, row, combos):
        for a, dc, dx in combos:
            number, tile, i = place.at(row, dx, CHUNKS[chunk][a], dc)
            pltpu.make_async_remote_copy(
                pair(outbox, tile, i), pair(inbox, first_tile(chunk) + dy * len(CHUNKS[chunk]) + a, dc * NX + dx),
                out_sem, in_sem.at[chunk], device_id=number, device_id_type=LOGICAL,
            ).start()

    pl.semaphore_wait(pltpu.get_barrier_semaphore(), NX * NY * NC + NZ - 2)
    for dz in range(1, NZ):
        pl.semaphore_signal(met.at[NZ - dz], inc=1, device_id=place.at(here, 0, dz, 0)[0], device_id_type=LOGICAL)
    for chunk in range(len(CHUNKS)):
        post(chunk, 0, here, [(a, 0, 0) for a in range(1 if chunk == 0 else 0, len(CHUNKS[chunk]))])
    post(0, 0, here, [(0, dc, dx) for dc, dx in PLANE if dc or dx])

    def post_row(dy, _):
        post(0, dy, place.row(dy), [(0, dc, dx) for dc, dx in PLANE])
        return 0

    lax.fori_loop(1, NY, post_row, 0)
    own = pltpu.make_async_copy(pair(outbox, me // 8, lax.rem(me, 8)), pair(inbox, 0, 0), in_sem.at[0])
    own.start()
    for chunk, group in GROUPS:
        for a in group:
            pl.semaphore_wait(met.at[CHUNKS[chunk][a]], 1)
        post(chunk, 0, here, [(a, dc, dx) for dc, dx in PLANE for a in group if dc or dx])

        def post_rest(dy, _):
            post(chunk, dy, place.row(dy), [(a, dc, dx) for dc, dx in PLANE for a in group])
            return 0

        lax.fori_loop(1, NY, post_rest, 0)
    load1.wait()
    load2.wait()

    near = place.at(here, 0, 0, 1)[0]
    for chunk in range(len(CHUNKS)):
        count = len(CHUNKS[chunk]) * PLANE_TILES
        tiles = pl.ds(first_tile(chunk), count)
        at_rows = pl.ds(0, count * ROWS)
        pltpu.make_async_remote_copy(
            inbox.at[tiles], inbox.at[tiles], out_sem, in_sem.at[chunk], device_id=near, device_id_type=LOGICAL
        ).wait_recv()
        rows = columns(inbox, tiles, count)

        def widen(k, _):
            at = pl.ds(pl.multiple_of(k * 256, 256), 256)
            h = jnp.dot(rows, w1[:, at], preferred_element_type=jnp.float32)
            hidden[at_rows, at] = jnp.maximum(h, 0.0).astype(jnp.bfloat16)
            return 0

        lax.fori_loop(0, w1.shape[1] // 256, widen, 0)
        for j in range(parts // 2):
            r = lax.dot_general(
                hidden[at_rows, :], w2[j * 256 : j * 256 + 256, :], (((1,), (1,)), ((), ())), preferred_element_type=jnp.float32
            ).astype(jnp.bfloat16)
            for half in range(2):
                results[tiles, 2 * j + half] = r[:, half * LANES : (half + 1) * LANES].reshape(count, ROWS, LANES)

        home = pair(returned, me // 8, lax.rem(me, 8))

        def reply(dy, row, combos):
            for a, dc, dx in combos:
                number = place.at(row, -dx % NX, -CHUNKS[chunk][a] % NZ, dc)[0]
                pltpu.make_async_remote_copy(
                    pair(results, first_tile(chunk) + dy * len(CHUNKS[chunk]) + a, dc * NX + dx), home,
                    back_sem, home_sem, device_id=number, device_id_type=LOGICAL,
                ).start()

        for a in range(len(CHUNKS[chunk])):
            reply(0, here, [(a, dc, dx) for dc, dx in PLANE if CHUNKS[chunk][a] or dc or dx])

            def reply_row(dy, _):
                reply(dy, place.row(NY - dy), [(a, dc, dx) for dc, dx in PLANE])
                return 0

            lax.fori_loop(1, NY, reply_row, 0)
        if chunk == 0:
            pltpu.make_async_copy(pair(results, 0, 0), home, home_sem).start()

    everything = pltpu.make_async_remote_copy(returned, returned, back_sem, home_sem, device_id=near, device_id_type=LOGICAL)
    everything.wait_recv()
    rest = columns(returned, slice(None), 2 * N // ROWS)
    picked = lax.dot_general(picks, rest, (((0,), (0,)), ((), ())), preferred_element_type=jnp.float32)
    weight = jnp.transpose(jnp.broadcast_to(gates[...], (LANES, n_tok)))
    weight = jnp.concatenate([weight] * parts, axis=1)
    gated[...] = weight * picked
    left = 2 * N // ROWS - 1
    for box, sem in ((outbox, out_sem), (results, back_sem)):
        pltpu.make_async_copy(box.at[pl.ds(0, left)], box.at[pl.ds(0, left)], sem).wait()
        pltpu.make_async_copy(box.at[0, :, pl.ds(0, ROWS - 2), :], box.at[0, :, pl.ds(0, ROWS - 2), :], sem).wait()


def local(tokens, norm_gain, gates, expert_ids, slots, w_in, w_out):
    n_tok, width = tokens.shape
    hidden = w_in.shape[2]
    box = pltpu.VMEM((2 * N // ROWS, width // LANES, ROWS, LANES), jnp.bfloat16)
    vmem, hbm = pl.BlockSpec(memory_space=pltpu.VMEM), pl.BlockSpec(memory_space=pltpu.HBM)
    gated = pl.pallas_call(
        kernel,
        out_shape=jax.ShapeDtypeStruct(tokens.shape, jnp.float32),
        in_specs=[hbm] * 7,
        out_specs=vmem,
        scratch_shapes=[
            pltpu.VMEM((n_tok, width), tokens.dtype),
            pltpu.VMEM((width,), jnp.float32),
            pltpu.VMEM((1, n_tok), jnp.float32),
            pltpu.VMEM((1, n_tok), jnp.int32),
            pltpu.VMEM((1, n_tok), jnp.int32),
            box, box, box, box,
            pltpu.VMEM((width, hidden), jnp.bfloat16),
            pltpu.VMEM((width, hidden), jnp.bfloat16),
            pltpu.VMEM((max(map(len, CHUNKS)) * PLANE_TILES * ROWS, hidden), jnp.bfloat16),
            pltpu.SemaphoreType.REGULAR((NZ,)),
            pltpu.SemaphoreType.DMA((5,)),
            pltpu.SemaphoreType.DMA((2,)),
            pltpu.SemaphoreType.DMA,
            pltpu.SemaphoreType.DMA((len(CHUNKS),)),
            pltpu.SemaphoreType.DMA,
            pltpu.SemaphoreType.DMA,
        ],
        compiler_params=pltpu.CompilerParams(collective_id=0, has_side_effects=True, vmem_limit_bytes=VMEM_LIMIT),
    )(*[pltpu.with_memory_space_constraint(v, pltpu.HBM) for v in (tokens, norm_gain, gates.reshape(1, n_tok), expert_ids.reshape(1, n_tok),
      slots.reshape(1, n_tok), w_in, w_out)])
    return (tokens.astype(jnp.float32) + gated).astype(tokens.dtype)


def solution(mesh):
    in_specs = (
        P(("expert", "tensor"), None),
        P(),
        P(("expert", "tensor")),
        P(("expert", "tensor")),
        P(("expert", "tensor")),
        P(("expert", "tensor"), None, None),
        P(("expert", "tensor"), None, None),
    )
    out_specs = P(("expert", "tensor"), None)
    return jax.shard_map(local, mesh=mesh, in_specs=in_specs, out_specs=out_specs, check_vma=False)
```

```python
import functools

import jax
import jax.numpy as jnp
from jax import lax
from jax.experimental import pallas as pl
from jax.experimental.pallas import tpu as pltpu
from jax.sharding import PartitionSpec as P

LOGICAL = pl.DeviceIdType.LOGICAL
NX, NY, NZ, NC = 4, 4, 8, 2
N = NX * NY * NZ * NC
LANES, ROWS = 128, 16
VMEM_LIMIT = 24 * 1024 * 1024
CHUNKS = ((0, 3, 5), (4, 1, 7), (2, 6))
PLANE_TILES = NX * NY * NC * 2 // ROWS
GROUPS = ((0, (1,)), (0, (2,)), (1, (1,)), (1, (2,)), (1, (0,)), (2, (0,)), (2, (1,)))
PLANE = [(dc, dx) for dc in range(NC) for dx in range(NX)]


def first_tile(chunk):
    return sum(map(len, CHUNKS[:chunk])) * PLANE_TILES


class Place:
    def __init__(self):
        e, t = lax.axis_index("expert"), lax.axis_index("tensor")
        core, z = lax.rem(e, NC), lax.rem(e // NC, NZ)
        y, xh = lax.rem(e // (NC * NZ), NY), e // (NC * NZ * NY)
        self.me = e * 2 + t
        self.y = y
        xs = [lax.rem(xh * 2 + t + d, NX) for d in range(NX)]
        zs = [lax.rem(z + d, NZ) for d in range(NZ)]
        cs = [lax.rem(core + d, NC) for d in range(NC)]
        self.along_x = [(x // 2 * 128 + lax.rem(x, 2), x // 2 * 16, lax.rem(x, 2)) for x in xs]
        self.along_z = [(z * 4, z // 2, lax.rem(z, 2) * 4) for z in zs]
        self.along_c = [(c * 2, c * 2) for c in cs]

    def row(self, dy):
        y = lax.rem(self.y + dy, NY)
        return y * 32, y * 4

    def at(self, row, dx, dz, dc):
        x, z, c = self.along_x[dx], self.along_z[dz], self.along_c[dc]
        return row[0] + z[0] + (x[0] + c[0]), row[1] + z[1] + x[1], z[2] + (x[2] + c[1])


def pair(ref, tile, i):
    return ref.at[tile, :, pl.ds(2 * i, 2), :]


def greet(place):
    barrier = pltpu.get_barrier_semaphore()
    rows = [place.row(dy) for dy in range(NY)]
    for dz in range(1, NZ):
        pl.semaphore_signal(barrier, inc=1, device_id=place.at(rows[0], 0, dz, 0)[0], device_id_type=LOGICAL)
    for dy in range(NY):
        for dc, dx in PLANE:
            if dy or dc or dx:
                pl.semaphore_signal(barrier, inc=1, device_id=place.at(rows[dy], dx, 0, dc)[0], device_id_type=LOGICAL)


def columns(ref, tiles, count):
    return jnp.concatenate([ref[tiles, j].reshape(count * ROWS, LANES) for j in range(ref.shape[1])], axis=1)


def kernel(tokens_hbm, gain_hbm, gates_hbm, ids_hbm, slots_hbm, w_in, w_out, gated,
           tokens, gain, gates, ids, slots, outbox, inbox, results, returned, w1, w2, hidden,
           met, arg_sem, w_sem, out_sem, in_sem, back_sem, home_sem):
    loads = [
        pltpu.make_async_copy(hbm, vmem, arg_sem.at[i])
        for i, (hbm, vmem) in enumerate(
            ((tokens_hbm, tokens), (gain_hbm, gain), (gates_hbm, gates), (ids_hbm, ids), (slots_hbm, slots))
        )
    ]
    for load in loads:
        load.start()
    place = Place()
    me = place.me
    n_tok, width = tokens.shape
    parts = width // LANES
    load1 = pltpu.make_async_copy(w_in.at[0], w1, w_sem.at[0])
    load2 = pltpu.make_async_copy(w_out.at[0], w2, w_sem.at[1])
    greet(place)
    for load in loads:
        load.wait()
    load1.start()
    load2.start()

    values = tokens[...].astype(jnp.float32)
    square = jnp.mean(values * values, axis=-1, keepdims=True)
    normed = (values * lax.rsqrt(square + 1e-06) * gain[...].reshape(1, width)).astype(jnp.bfloat16)
    index = jnp.where(slots[...] >= 0, ids[...] * 2 + slots[...], -1)
    picks = (lax.broadcasted_iota(jnp.int32, (2 * N, n_tok), 0) == index).astype(jnp.bfloat16)
    for j in range(parts // 2):
        block = jnp.dot(picks, normed[:, j * 256 : j * 256 + 256], preferred_element_type=jnp.float32).astype(jnp.bfloat16)
        for half in range(2):
            outbox[:, 2 * j + half] = block[:, half * LANES : (half + 1) * LANES].reshape(2 * N // ROWS, ROWS, LANES)

    here = place.row(0)

    def post(chunk, dy, row, combos):
        for a, dc, dx in combos:
            number, tile, i = place.at(row, dx, CHUNKS[chunk][a], dc)
            pltpu.make_async_remote_copy(
                pair(outbox, tile, i), pair(inbox, first_tile(chunk) + dy * len(CHUNKS[chunk]) + a, dc * NX + dx),
                out_sem, in_sem.at[chunk], device_id=number, device_id_type=LOGICAL,
            ).start()

    pl.semaphore_wait(pltpu.get_barrier_semaphore(), NX * NY * NC + NZ - 2)
    for dz in range(1, NZ):
        pl.semaphore_signal(met.at[NZ - dz], inc=1, device_id=place.at(here, 0, dz, 0)[0], device_id_type=LOGICAL)
    for chunk in range(len(CHUNKS)):
        post(chunk, 0, here, [(a, 0, 0) for a in range(1 if chunk == 0 else 0, len(CHUNKS[chunk]))])
    post(0, 0, here, [(0, dc, dx) for dc, dx in PLANE if dc or dx])

    def post_row(dy, _):
        post(0, dy, place.row(dy), [(0, dc, dx) for dc, dx in PLANE])
        return 0

    lax.fori_loop(1, NY, post_row, 0)
    own = pltpu.make_async_copy(pair(outbox, me // 8, lax.rem(me, 8)), pair(inbox, 0, 0), in_sem.at[0])
    own.start()
    for chunk, group in GROUPS:
        for a in group:
            pl.semaphore_wait(met.at[CHUNKS[chunk][a]], 1)
        post(chunk, 0, here, [(a, dc, dx) for dc, dx in PLANE for a in group if dc or dx])

        def post_rest(dy, _):
            post(chunk, dy, place.row(dy), [(a, dc, dx) for dc, dx in PLANE for a in group])
            return 0

        lax.fori_loop(1, NY, post_rest, 0)
    load1.wait()
    load2.wait()

    near = place.at(here, 0, 0, 1)[0]
    for chunk in range(len(CHUNKS)):
        count = len(CHUNKS[chunk]) * PLANE_TILES
        tiles = pl.ds(first_tile(chunk), count)
        at_rows = pl.ds(0, count * ROWS)
        pltpu.make_async_remote_copy(
            inbox.at[tiles], inbox.at[tiles], out_sem, in_sem.at[chunk], device_id=near, device_id_type=LOGICAL
        ).wait_recv()
        rows = columns(inbox, tiles, count)

        def widen(k, _):
            at = pl.ds(pl.multiple_of(k * 512, 512), 512)
            h = jnp.dot(rows, w1[:, at], preferred_element_type=jnp.float32)
            hidden[at_rows, at] = jnp.maximum(h, 0.0).astype(jnp.bfloat16)
            return 0

        lax.fori_loop(0, w1.shape[1] // 512, widen, 0)
        for j in range(parts // 2):
            r = lax.dot_general(
                hidden[at_rows, :], w2[j * 256 : j * 256 + 256, :], (((1,), (1,)), ((), ())), preferred_element_type=jnp.float32
            ).astype(jnp.bfloat16)
            for half in range(2):
                results[tiles, 2 * j + half] = r[:, half * LANES : (half + 1) * LANES].reshape(count, ROWS, LANES)

        home = pair(returned, me // 8, lax.rem(me, 8))

        def reply(dy, row, combos):
            for a, dc, dx in combos:
                number = place.at(row, -dx % NX, -CHUNKS[chunk][a] % NZ, dc)[0]
                pltpu.make_async_remote_copy(
                    pair(results, first_tile(chunk) + dy * len(CHUNKS[chunk]) + a, dc * NX + dx), home,
                    back_sem, home_sem, device_id=number, device_id_type=LOGICAL,
                ).start()

        for a in range(len(CHUNKS[chunk])):
            reply(0, here, [(a, dc, dx) for dc, dx in PLANE if CHUNKS[chunk][a] or dc or dx])

            def reply_row(dy, _):
                reply(dy, place.row(NY - dy), [(a, dc, dx) for dc, dx in PLANE])
                return 0

            lax.fori_loop(1, NY, reply_row, 0)
        if chunk == 0:
            pltpu.make_async_copy(pair(results, 0, 0), home, home_sem).start()

    everything = pltpu.make_async_remote_copy(returned, returned, back_sem, home_sem, device_id=near, device_id_type=LOGICAL)
    everything.wait_recv()
    rest = columns(returned, slice(None), 2 * N // ROWS)
    picked = lax.dot_general(picks, rest, (((0,), (0,)), ((), ())), preferred_element_type=jnp.float32)
    weight = jnp.transpose(jnp.broadcast_to(gates[...], (LANES, n_tok)))
    weight = jnp.concatenate([weight] * parts, axis=1)
    gated[...] = weight * picked
    left = 2 * N // ROWS - 1
    for box, sem in ((outbox, out_sem), (results, back_sem)):
        pltpu.make_async_copy(box.at[pl.ds(0, left)], box.at[pl.ds(0, left)], sem).wait()
        pltpu.make_async_copy(box.at[0, :, pl.ds(0, ROWS - 2), :], box.at[0, :, pl.ds(0, ROWS - 2), :], sem).wait()


def local(tokens, norm_gain, gates, expert_ids, slots, w_in, w_out):
    n_tok, width = tokens.shape
    hidden = w_in.shape[2]
    box = pltpu.VMEM((2 * N // ROWS, width // LANES, ROWS, LANES), jnp.bfloat16)
    vmem, hbm = pl.BlockSpec(memory_space=pltpu.VMEM), pl.BlockSpec(memory_space=pltpu.HBM)
    gated = pl.pallas_call(
        kernel,
        out_shape=jax.ShapeDtypeStruct(tokens.shape, jnp.float32),
        in_specs=[hbm] * 7,
        out_specs=vmem,
        scratch_shapes=[
            pltpu.VMEM((n_tok, width), tokens.dtype),
            pltpu.VMEM((width,), jnp.float32),
            pltpu.VMEM((1, n_tok), jnp.float32),
            pltpu.VMEM((1, n_tok), jnp.int32),
            pltpu.VMEM((1, n_tok), jnp.int32),
            box, box, box, box,
            pltpu.VMEM((width, hidden), jnp.bfloat16),
            pltpu.VMEM((width, hidden), jnp.bfloat16),
            pltpu.VMEM((max(map(len, CHUNKS)) * PLANE_TILES * ROWS, hidden), jnp.bfloat16),
            pltpu.SemaphoreType.REGULAR((NZ,)),
            pltpu.SemaphoreType.DMA((5,)),
            pltpu.SemaphoreType.DMA((2,)),
            pltpu.SemaphoreType.DMA,
            pltpu.SemaphoreType.DMA((len(CHUNKS),)),
            pltpu.SemaphoreType.DMA,
            pltpu.SemaphoreType.DMA,
        ],
        compiler_params=pltpu.CompilerParams(collective_id=0, has_side_effects=True, vmem_limit_bytes=VMEM_LIMIT),
    )(*[pltpu.with_memory_space_constraint(v, pltpu.HBM) for v in (tokens, norm_gain, gates.reshape(1, n_tok), expert_ids.reshape(1, n_tok),
      slots.reshape(1, n_tok), w_in, w_out)])
    return (tokens.astype(jnp.float32) + gated).astype(tokens.dtype)


def solution(mesh):
    in_specs = (
        P(("expert", "tensor"), None),
        P(),
        P(("expert", "tensor")),
        P(("expert", "tensor")),
        P(("expert", "tensor")),
        P(("expert", "tensor"), None, None),
        P(("expert", "tensor"), None, None),
    )
    out_specs = P(("expert", "tensor"), None)
    return jax.shard_map(local, mesh=mesh, in_specs=in_specs, out_specs=out_specs, check_vma=False)
```

```python
import functools

import jax
import jax.numpy as jnp
from jax import lax
from jax.experimental import pallas as pl
from jax.experimental.pallas import tpu as pltpu
from jax.sharding import PartitionSpec as P

LOGICAL = pl.DeviceIdType.LOGICAL
NX, NY, NZ, NC = 4, 4, 8, 2
N = NX * NY * NZ * NC
LANES, ROWS = 128, 16
VMEM_LIMIT = 24 * 1024 * 1024
CHUNKS = ((0, 3, 5), (4, 1, 7), (2, 6))
PLANE_TILES = NX * NY * NC * 2 // ROWS
GROUPS = ((0, (1,)), (0, (2,)), (1, (1,)), (1, (2,)), (1, (0,)), (2, (0,)), (2, (1,)))
PLANE = [(dc, dx) for dc in range(NC) for dx in range(NX)]


def first_tile(chunk):
    return sum(map(len, CHUNKS[:chunk])) * PLANE_TILES


class Place:
    def __init__(self):
        e, t = lax.axis_index("expert"), lax.axis_index("tensor")
        core, z = lax.rem(e, NC), lax.rem(e // NC, NZ)
        y, xh = lax.rem(e // (NC * NZ), NY), e // (NC * NZ * NY)
        self.me = e * 2 + t
        self.y = y
        xs = [lax.rem(xh * 2 + t + d, NX) for d in range(NX)]
        zs = [lax.rem(z + d, NZ) for d in range(NZ)]
        cs = [lax.rem(core + d, NC) for d in range(NC)]
        self.along_x = [(x // 2 * 128 + lax.rem(x, 2), x // 2 * 16, lax.rem(x, 2)) for x in xs]
        self.along_z = [(z * 4, z // 2, lax.rem(z, 2) * 4) for z in zs]
        self.along_c = [(c * 2, c * 2) for c in cs]

    def row(self, dy):
        y = lax.rem(self.y + dy, NY)
        return y * 32, y * 4

    def at(self, row, dx, dz, dc):
        x, z, c = self.along_x[dx], self.along_z[dz], self.along_c[dc]
        return row[0] + z[0] + (x[0] + c[0]), row[1] + z[1] + x[1], z[2] + (x[2] + c[1])


def pair(ref, tile, i):
    return ref.at[tile, :, pl.ds(2 * i, 2), :]


def greet(place):
    barrier = pltpu.get_barrier_semaphore()
    rows = [place.row(dy) for dy in range(NY)]
    for dz in (4, 3, 5, 2, 6, 1, 7):
        pl.semaphore_signal(barrier, inc=1, device_id=place.at(rows[0], 0, dz, 0)[0], device_id_type=LOGICAL)
    for dy in range(NY):
        for dc, dx in PLANE:
            if dy or dc or dx:
                pl.semaphore_signal(barrier, inc=1, device_id=place.at(rows[dy], dx, 0, dc)[0], device_id_type=LOGICAL)


def columns(ref, tiles, count):
    return jnp.concatenate([ref[tiles, j].reshape(count * ROWS, LANES) for j in range(ref.shape[1])], axis=1)


def kernel(tokens_hbm, gain_hbm, gates_hbm, ids_hbm, slots_hbm, w_in, w_out, gated,
           tokens, gain, gates, ids, slots, outbox, inbox, results, returned, w1, w2, hidden,
           met, arg_sem, w_sem, out_sem, in_sem, back_sem, home_sem):
    loads = [
        pltpu.make_async_copy(hbm, vmem, arg_sem.at[i])
        for i, (hbm, vmem) in enumerate(
            ((tokens_hbm, tokens), (gain_hbm, gain), (gates_hbm, gates), (ids_hbm, ids), (slots_hbm, slots))
        )
    ]
    for load in loads:
        load.start()
    place = Place()
    me = place.me
    n_tok, width = tokens.shape
    parts = width // LANES
    load1 = pltpu.make_async_copy(w_in.at[0], w1, w_sem.at[0])
    load2 = pltpu.make_async_copy(w_out.at[0], w2, w_sem.at[1])
    greet(place)
    for load in loads:
        load.wait()
    load1.start()
    load2.start()

    values = tokens[...].astype(jnp.float32)
    square = jnp.mean(values * values, axis=-1, keepdims=True)
    normed = (values * lax.rsqrt(square + 1e-06) * gain[...].reshape(1, width)).astype(jnp.bfloat16)
    index = jnp.where(slots[...] >= 0, ids[...] * 2 + slots[...], -1)
    picks = (lax.broadcasted_iota(jnp.int32, (2 * N, n_tok), 0) == index).astype(jnp.bfloat16)
    for j in range(parts // 2):
        block = jnp.dot(picks, normed[:, j * 256 : j * 256 + 256], preferred_element_type=jnp.float32).astype(jnp.bfloat16)
        for half in range(2):
            outbox[:, 2 * j + half] = block[:, half * LANES : (half + 1) * LANES].reshape(2 * N // ROWS, ROWS, LANES)

    here = place.row(0)

    def post(chunk, dy, row, combos):
        for a, dc, dx in combos:
            number, tile, i = place.at(row, dx, CHUNKS[chunk][a], dc)
            pltpu.make_async_remote_copy(
                pair(outbox, tile, i), pair(inbox, first_tile(chunk) + dy * len(CHUNKS[chunk]) + a, dc * NX + dx),
                out_sem, in_sem.at[chunk], device_id=number, device_id_type=LOGICAL,
            ).start()

    pl.semaphore_wait(pltpu.get_barrier_semaphore(), NX * NY * NC + NZ - 2)
    for dz in (5, 3, 7, 1, 4, 6, 2):
        pl.semaphore_signal(met.at[NZ - dz], inc=1, device_id=place.at(here, 0, dz, 0)[0], device_id_type=LOGICAL)
    for chunk in range(len(CHUNKS)):
        post(chunk, 0, here, [(a, 0, 0) for a in range(1 if chunk == 0 else 0, len(CHUNKS[chunk]))])
    post(0, 0, here, [(0, dc, dx) for dc, dx in PLANE if dc or dx])

    def post_row(dy, _):
        post(0, dy, place.row(dy), [(0, dc, dx) for dc, dx in PLANE])
        return 0

    lax.fori_loop(1, NY, post_row, 0)
    own = pltpu.make_async_copy(pair(outbox, me // 8, lax.rem(me, 8)), pair(inbox, 0, 0), in_sem.at[0])
    own.start()
    for chunk, group in GROUPS:
        for a in group:
            pl.semaphore_wait(met.at[CHUNKS[chunk][a]], 1)
        post(chunk, 0, here, [(a, dc, dx) for dc, dx in PLANE for a in group if dc or dx])

        def post_rest(dy, _):
            post(chunk, dy, place.row(dy), [(a, dc, dx) for dc, dx in PLANE for a in group])
            return 0

        lax.fori_loop(1, NY, post_rest, 0)
    load1.wait()
    load2.wait()

    near = place.at(here, 0, 0, 1)[0]
    for chunk in range(len(CHUNKS)):
        count = len(CHUNKS[chunk]) * PLANE_TILES
        tiles = pl.ds(first_tile(chunk), count)
        at_rows = pl.ds(0, count * ROWS)
        pltpu.make_async_remote_copy(
            inbox.at[tiles], inbox.at[tiles], out_sem, in_sem.at[chunk], device_id=near, device_id_type=LOGICAL
        ).wait_recv()
        rows = columns(inbox, tiles, count)

        def widen(k, _):
            at = pl.ds(pl.multiple_of(k * 512, 512), 512)
            h = jnp.dot(rows, w1[:, at], preferred_element_type=jnp.float32)
            hidden[at_rows, at] = jnp.maximum(h, 0.0).astype(jnp.bfloat16)
            return 0

        lax.fori_loop(0, w1.shape[1] // 512, widen, 0)
        for j in range(parts // 2):
            r = lax.dot_general(
                hidden[at_rows, :], w2[j * 256 : j * 256 + 256, :], (((1,), (1,)), ((), ())), preferred_element_type=jnp.float32
            ).astype(jnp.bfloat16)
            for half in range(2):
                results[tiles, 2 * j + half] = r[:, half * LANES : (half + 1) * LANES].reshape(count, ROWS, LANES)

        home = pair(returned, me // 8, lax.rem(me, 8))

        def reply(dy, row, combos):
            for a, dc, dx in combos:
                number = place.at(row, -dx % NX, -CHUNKS[chunk][a] % NZ, dc)[0]
                pltpu.make_async_remote_copy(
                    pair(results, first_tile(chunk) + dy * len(CHUNKS[chunk]) + a, dc * NX + dx), home,
                    back_sem, home_sem, device_id=number, device_id_type=LOGICAL,
                ).start()

        for a in range(len(CHUNKS[chunk])):
            reply(0, here, [(a, dc, dx) for dc, dx in PLANE if CHUNKS[chunk][a] or dc or dx])

            def reply_row(dy, _):
                reply(dy, place.row(NY - dy), [(a, dc, dx) for dc, dx in PLANE])
                return 0

            lax.fori_loop(1, NY, reply_row, 0)
        if chunk == 0:
            pltpu.make_async_copy(pair(results, 0, 0), home, home_sem).start()

    everything = pltpu.make_async_remote_copy(returned, returned, back_sem, home_sem, device_id=near, device_id_type=LOGICAL)
    everything.wait_recv()
    rest = columns(returned, slice(None), 2 * N // ROWS)
    picked = lax.dot_general(picks, rest, (((0,), (0,)), ((), ())), preferred_element_type=jnp.float32)
    weight = jnp.transpose(jnp.broadcast_to(gates[...], (LANES, n_tok)))
    weight = jnp.concatenate([weight] * parts, axis=1)
    gated[...] = weight * picked
    left = 2 * N // ROWS - 1
    for box, sem in ((outbox, out_sem), (results, back_sem)):
        pltpu.make_async_copy(box.at[pl.ds(0, left)], box.at[pl.ds(0, left)], sem).wait()
        pltpu.make_async_copy(box.at[0, :, pl.ds(0, ROWS - 2), :], box.at[0, :, pl.ds(0, ROWS - 2), :], sem).wait()


def local(tokens, norm_gain, gates, expert_ids, slots, w_in, w_out):
    n_tok, width = tokens.shape
    hidden = w_in.shape[2]
    box = pltpu.VMEM((2 * N // ROWS, width // LANES, ROWS, LANES), jnp.bfloat16)
    vmem, hbm = pl.BlockSpec(memory_space=pltpu.VMEM), pl.BlockSpec(memory_space=pltpu.HBM)
    gated = pl.pallas_call(
        kernel,
        out_shape=jax.ShapeDtypeStruct(tokens.shape, jnp.float32),
        in_specs=[hbm] * 7,
        out_specs=vmem,
        scratch_shapes=[
            pltpu.VMEM((n_tok, width), tokens.dtype),
            pltpu.VMEM((width,), jnp.float32),
            pltpu.VMEM((1, n_tok), jnp.float32),
            pltpu.VMEM((1, n_tok), jnp.int32),
            pltpu.VMEM((1, n_tok), jnp.int32),
            box, box, box, box,
            pltpu.VMEM((width, hidden), jnp.bfloat16),
            pltpu.VMEM((width, hidden), jnp.bfloat16),
            pltpu.VMEM((max(map(len, CHUNKS)) * PLANE_TILES * ROWS, hidden), jnp.bfloat16),
            pltpu.SemaphoreType.REGULAR((NZ,)),
            pltpu.SemaphoreType.DMA((5,)),
            pltpu.SemaphoreType.DMA((2,)),
            pltpu.SemaphoreType.DMA,
            pltpu.SemaphoreType.DMA((len(CHUNKS),)),
            pltpu.SemaphoreType.DMA,
            pltpu.SemaphoreType.DMA,
        ],
        compiler_params=pltpu.CompilerParams(collective_id=0, has_side_effects=True, vmem_limit_bytes=VMEM_LIMIT),
    )(*[pltpu.with_memory_space_constraint(v, pltpu.HBM) for v in (tokens, norm_gain, gates.reshape(1, n_tok), expert_ids.reshape(1, n_tok),
      slots.reshape(1, n_tok), w_in, w_out)])
    return (tokens.astype(jnp.float32) + gated).astype(tokens.dtype)


def solution(mesh):
    in_specs = (
        P(("expert", "tensor"), None),
        P(),
        P(("expert", "tensor")),
        P(("expert", "tensor")),
        P(("expert", "tensor")),
        P(("expert", "tensor"), None, None),
        P(("expert", "tensor"), None, None),
    )
    out_specs = P(("expert", "tensor"), None)
    return jax.shard_map(local, mesh=mesh, in_specs=in_specs, out_specs=out_specs, check_vma=False)
```

```python
import functools

import jax
import jax.numpy as jnp
from jax import lax
from jax.experimental import pallas as pl
from jax.experimental.pallas import tpu as pltpu
from jax.sharding import PartitionSpec as P

LOGICAL = pl.DeviceIdType.LOGICAL
NX, NY, NZ, NC = 4, 4, 8, 2
N = NX * NY * NZ * NC
LANES, ROWS = 128, 16
VMEM_LIMIT = 24 * 1024 * 1024
CHUNKS = ((0, 3, 5), (4, 1, 7), (2, 6))
PLANE_TILES = NX * NY * NC * 2 // ROWS
GROUPS = ((0, (1,)), (0, (2,)), (1, (1,)), (1, (2,)), (1, (0,)), (2, (0,)), (2, (1,)))
PLANE = [(dc, dx) for dc in range(NC) for dx in range(NX)]


def first_tile(chunk):
    return sum(map(len, CHUNKS[:chunk])) * PLANE_TILES


class Place:
    def __init__(self):
        e, t = lax.axis_index("expert"), lax.axis_index("tensor")
        core, z = lax.rem(e, NC), lax.rem(e // NC, NZ)
        y, xh = lax.rem(e // (NC * NZ), NY), e // (NC * NZ * NY)
        self.me = e * 2 + t
        self.y = y
        xs = [lax.rem(xh * 2 + t + d, NX) for d in range(NX)]
        zs = [lax.rem(z + d, NZ) for d in range(NZ)]
        cs = [lax.rem(core + d, NC) for d in range(NC)]
        self.along_x = [(x // 2 * 128 + lax.rem(x, 2), x // 2 * 16, lax.rem(x, 2)) for x in xs]
        self.along_z = [(z * 4, z // 2, lax.rem(z, 2) * 4) for z in zs]
        self.along_c = [(c * 2, c * 2) for c in cs]

    def row(self, dy):
        y = lax.rem(self.y + dy, NY)
        return y * 32, y * 4

    def at(self, row, dx, dz, dc):
        x, z, c = self.along_x[dx], self.along_z[dz], self.along_c[dc]
        return row[0] + z[0] + (x[0] + c[0]), row[1] + z[1] + x[1], z[2] + (x[2] + c[1])


def pair(ref, tile, i):
    return ref.at[tile, :, pl.ds(2 * i, 2), :]


def greet(place):
    barrier = pltpu.get_barrier_semaphore()
    rows = [place.row(dy) for dy in range(NY)]
    for dz in range(1, NZ):
        pl.semaphore_signal(barrier, inc=1, device_id=place.at(rows[0], 0, dz, 0)[0], device_id_type=LOGICAL)
    for dy in range(NY):
        for dc, dx in PLANE:
            if dy or dc or dx:
                pl.semaphore_signal(barrier, inc=1, device_id=place.at(rows[dy], dx, 0, dc)[0], device_id_type=LOGICAL)


def columns(ref, tiles, count):
    return jnp.concatenate([ref[tiles, j].reshape(count * ROWS, LANES) for j in range(ref.shape[1])], axis=1)


def kernel(tokens_hbm, gain_hbm, gates_hbm, ids_hbm, slots_hbm, w_in, w_out, gated,
           tokens, gain, gates, ids, slots, outbox, inbox, results, returned, w1, w2, hidden,
           met, arg_sem, w_sem, out_sem, in_sem, back_sem, home_sem):
    loads = [
        pltpu.make_async_copy(hbm, vmem, arg_sem.at[i])
        for i, (hbm, vmem) in enumerate(
            ((tokens_hbm, tokens), (gain_hbm, gain), (gates_hbm, gates), (ids_hbm, ids), (slots_hbm, slots))
        )
    ]
    for load in loads:
        load.start()
    place = Place()
    me = place.me
    n_tok, width = tokens.shape
    parts = width // LANES
    load1 = pltpu.make_async_copy(w_in.at[0], w1, w_sem.at[0])
    load2 = pltpu.make_async_copy(w_out.at[0], w2, w_sem.at[1])
    greet(place)
    for load in loads:
        load.wait()
    load1.start()
    load2.start()

    values = tokens[...].astype(jnp.float32)
    square = jnp.mean(values * values, axis=-1, keepdims=True)
    normed = (values * lax.rsqrt(square + 1e-06) * gain[...].reshape(1, width)).astype(jnp.bfloat16)
    index = jnp.where(slots[...] >= 0, ids[...] * 2 + slots[...], -1)
    picks = (lax.broadcasted_iota(jnp.int32, (2 * N, n_tok), 0) == index).astype(jnp.bfloat16)
    for j in range(parts // 2):
        block = jnp.dot(picks, normed[:, j * 256 : j * 256 + 256], preferred_element_type=jnp.float32).astype(jnp.bfloat16)
        for half in range(2):
            outbox[:, 2 * j + half] = block[:, half * LANES : (half + 1) * LANES].reshape(2 * N // ROWS, ROWS, LANES)

    here = place.row(0)

    def post(chunk, dy, row, combos):
        for a, dc, dx in combos:
            number, tile, i = place.at(row, dx, CHUNKS[chunk][a], dc)
            pltpu.make_async_remote_copy(
                pair(outbox, tile, i), pair(inbox, first_tile(chunk) + dy * len(CHUNKS[chunk]) + a, dc * NX + dx),
                out_sem, in_sem.at[chunk], device_id=number, device_id_type=LOGICAL,
            ).start()

    pl.semaphore_wait(pltpu.get_barrier_semaphore(), NX * NY * NC + NZ - 2)
    for dz in range(1, NZ):
        pl.semaphore_signal(met.at[NZ - dz], inc=1, device_id=place.at(here, 0, dz, 0)[0], device_id_type=LOGICAL)
    for chunk in range(len(CHUNKS)):
        post(chunk, 0, here, [(a, 0, 0) for a in range(1 if chunk == 0 else 0, len(CHUNKS[chunk]))])
    post(0, 0, here, [(0, dc, dx) for dc, dx in PLANE if dc or dx])

    def post_row(dy, _):
        post(0, dy, place.row(dy), [(0, dc, dx) for dc, dx in PLANE])
        return 0

    lax.fori_loop(1, NY, post_row, 0)
    own = pltpu.make_async_copy(pair(outbox, me // 8, lax.rem(me, 8)), pair(inbox, 0, 0), in_sem.at[0])
    own.start()
    for chunk, group in GROUPS:
        for a in group:
            pl.semaphore_wait(met.at[CHUNKS[chunk][a]], 1)
        post(chunk, 0, here, [(a, dc, dx) for dc, dx in PLANE for a in group if dc or dx])

        def post_rest(dy, _):
            post(chunk, dy, place.row(dy), [(a, dc, dx) for dc, dx in PLANE for a in group])
            return 0

        lax.fori_loop(1, NY, post_rest, 0)
    load1.wait()
    load2.wait()

    near = place.at(here, 0, 0, 1)[0]
    for chunk in range(len(CHUNKS)):
        count = len(CHUNKS[chunk]) * PLANE_TILES
        tiles = pl.ds(first_tile(chunk), count)
        at_rows = pl.ds(0, count * ROWS)
        pltpu.make_async_remote_copy(
            inbox.at[tiles], inbox.at[tiles], out_sem, in_sem.at[chunk], device_id=near, device_id_type=LOGICAL
        ).wait_recv()
        rows = columns(inbox, tiles, count)

        def widen(k, _):
            at = pl.ds(pl.multiple_of(k * 512, 512), 512)
            h = jnp.dot(rows, w1[:, at], preferred_element_type=jnp.float32)
            hidden[at_rows, at] = jnp.maximum(h, 0.0).astype(jnp.bfloat16)
            return 0

        lax.fori_loop(0, w1.shape[1] // 512, widen, 0)
        for j in range(0, parts, 6):
            r = lax.dot_general(
                hidden[at_rows, :], w2[j * LANES : (j + 6) * LANES, :], (((1,), (1,)), ((), ())), preferred_element_type=jnp.float32
            ).astype(jnp.bfloat16)
            for part in range(6):
                results[tiles, j + part] = r[:, part * LANES : (part + 1) * LANES].reshape(count, ROWS, LANES)

        home = pair(returned, me // 8, lax.rem(me, 8))

        def reply(dy, row, combos):
            for a, dc, dx in combos:
                number = place.at(row, -dx % NX, -CHUNKS[chunk][a] % NZ, dc)[0]
                pltpu.make_async_remote_copy(
                    pair(results, first_tile(chunk) + dy * len(CHUNKS[chunk]) + a, dc * NX + dx), home,
                    back_sem, home_sem, device_id=number, device_id_type=LOGICAL,
                ).start()

        for a in range(len(CHUNKS[chunk])):
            reply(0, here, [(a, dc, dx) for dc, dx in PLANE if CHUNKS[chunk][a] or dc or dx])

            def reply_row(dy, _):
                reply(dy, place.row(NY - dy), [(a, dc, dx) for dc, dx in PLANE])
                return 0

            lax.fori_loop(1, NY, reply_row, 0)
        if chunk == 0:
            pltpu.make_async_copy(pair(results, 0, 0), home, home_sem).start()

    everything = pltpu.make_async_remote_copy(returned, returned, back_sem, home_sem, device_id=near, device_id_type=LOGICAL)
    everything.wait_recv()
    rest = columns(returned, slice(None), 2 * N // ROWS)
    picked = lax.dot_general(picks, rest, (((0,), (0,)), ((), ())), preferred_element_type=jnp.float32)
    weight = jnp.transpose(jnp.broadcast_to(gates[...], (LANES, n_tok)))
    weight = jnp.concatenate([weight] * parts, axis=1)
    gated[...] = weight * picked
    left = 2 * N // ROWS - 1
    for box, sem in ((outbox, out_sem), (results, back_sem)):
        pltpu.make_async_copy(box.at[pl.ds(0, left)], box.at[pl.ds(0, left)], sem).wait()
        pltpu.make_async_copy(box.at[0, :, pl.ds(0, ROWS - 2), :], box.at[0, :, pl.ds(0, ROWS - 2), :], sem).wait()


def local(tokens, norm_gain, gates, expert_ids, slots, w_in, w_out):
    n_tok, width = tokens.shape
    hidden = w_in.shape[2]
    box = pltpu.VMEM((2 * N // ROWS, width // LANES, ROWS, LANES), jnp.bfloat16)
    vmem, hbm = pl.BlockSpec(memory_space=pltpu.VMEM), pl.BlockSpec(memory_space=pltpu.HBM)
    gated = pl.pallas_call(
        kernel,
        out_shape=jax.ShapeDtypeStruct(tokens.shape, jnp.float32),
        in_specs=[hbm] * 7,
        out_specs=vmem,
        scratch_shapes=[
            pltpu.VMEM((n_tok, width), tokens.dtype),
            pltpu.VMEM((width,), jnp.float32),
            pltpu.VMEM((1, n_tok), jnp.float32),
            pltpu.VMEM((1, n_tok), jnp.int32),
            pltpu.VMEM((1, n_tok), jnp.int32),
            box, box, box, box,
            pltpu.VMEM((width, hidden), jnp.bfloat16),
            pltpu.VMEM((width, hidden), jnp.bfloat16),
            pltpu.VMEM((max(map(len, CHUNKS)) * PLANE_TILES * ROWS, hidden), jnp.bfloat16),
            pltpu.SemaphoreType.REGULAR((NZ,)),
            pltpu.SemaphoreType.DMA((5,)),
            pltpu.SemaphoreType.DMA((2,)),
            pltpu.SemaphoreType.DMA,
            pltpu.SemaphoreType.DMA((len(CHUNKS),)),
            pltpu.SemaphoreType.DMA,
            pltpu.SemaphoreType.DMA,
        ],
        compiler_params=pltpu.CompilerParams(collective_id=0, has_side_effects=True, vmem_limit_bytes=VMEM_LIMIT),
    )(*[pltpu.with_memory_space_constraint(v, pltpu.HBM) for v in (tokens, norm_gain, gates.reshape(1, n_tok), expert_ids.reshape(1, n_tok),
      slots.reshape(1, n_tok), w_in, w_out)])
    return (tokens.astype(jnp.float32) + gated).astype(tokens.dtype)


def solution(mesh):
    in_specs = (
        P(("expert", "tensor"), None),
        P(),
        P(("expert", "tensor")),
        P(("expert", "tensor")),
        P(("expert", "tensor")),
        P(("expert", "tensor"), None, None),
        P(("expert", "tensor"), None, None),
    )
    out_specs = P(("expert", "tensor"), None)
    return jax.shard_map(local, mesh=mesh, in_specs=in_specs, out_specs=out_specs, check_vma=False)
```
